32 devices in a mesh: group: 8 (over y, x, core), resp: 4 (over z).
Axes of the slice: x: 2, y: 2, z: 4, core: 2. Of those that a mesh axis runs over, the one named last changes fastest.
Arguments:
- prompt_hidden: bfloat16 [8, 32, 4096], P('group', 'resp'), may hold values from -6 to 6
- kv_weight: bfloat16 [2048, 4096], P('resp'), may hold values from -0.09375 to 0.09375
- queries: bfloat16 [8, 512, 4096], P('group', 'resp'), may hold values from -150 to 150
- resp_keys: bfloat16 [8, 512, 1024], P('group', 'resp'), may hold values from -5 to 5
- resp_values: bfloat16 [8, 512, 1024], P('group', 'resp'), may hold values from -6 to 6
- upstream: bfloat16 [8, 512, 4096], P('group', 'resp'), may hold values from -6 to 6
- signs: int32 [8, 512], P('group', 'resp'), may hold values from -1 to 1
- lengths: int32 [8, 4], P('group', 'resp'), may hold values from 64 to 128
Outputs:
- grad_keys: bfloat16 [8, 512, 1024], P('group', 'resp')
- grad_values: bfloat16 [8, 512, 1024], P('group', 'resp')
- grad_weight: float32 [2048, 4096], P('resp', 'group')
The draws below stay inside these ranges and needn't reach their ends.
All inputs are finite; a program needn't handle non-finite values.
Results may differ from the reference program's by a relative error of at most 0.025.
Values may be sent and summed in bfloat16 or wider, within the bound.
No kernel may reach another device: no remote copies, remote signals or barrier semaphores. Data moves between devices by JAX's collectives and lax.ppermute only.
A program may use at most 64 MiB of HBM per device.

```python
import math
import jax
import jax.numpy as jnp
from jax import lax

D = 4096
HEADS = 32
KV_HEADS = 8
HEAD = 128
R_DEV = 128
QW = 4096
KVW = 1024
RESPONSES = 4
GROUPS = 8
PROMPT = 32
TOK_RESP = 512


def shared_draw(key):
    base_key = jax.random.fold_in(key, 7)
    key_width = KV_HEADS * HEAD
    key_rows = jnp.clip(jax.random.normal(jax.random.fold_in(base_key, 1), (GROUPS, TOK_RESP, key_width), jnp.float32), -5.0, 5.0)
    query_rows = jnp.clip(jax.random.normal(jax.random.fold_in(base_key, 2), (GROUPS, TOK_RESP, HEADS * HEAD), jnp.float32), -5.0, 5.0)
    return (key_rows, query_rows)


def draw_resp_keys(key, part):
    return shared_draw(key)[0].astype(jnp.bfloat16)


def draw_queries(key, part):
    return shared_draw(key)[1].astype(jnp.bfloat16)


def place_ends(result, rng, smallest, high):
    longest = result.shape.index(max(result.shape))
    spots = []
    for shift in (0, 1):
        where = [jax.random.randint(jax.random.fold_in(rng, axis), (), 0, length) for axis, length in enumerate(result.shape)]
        where[longest] = (where[longest] + shift) % result.shape[longest]
        spots.append(tuple(where))
    return result.at[spots[0]].set(smallest).at[spots[1]].set(high)


def strengthened(entries, key, source, target, blocks, factor):
    def block_of(axis_at):
        return (jnp.arange(entries.shape[axis_at]) // (entries.shape[axis_at] // blocks)).reshape((-1,) + (1,) * (entries.ndim - 1 - axis_at))

    near = jax.random.permutation(key, blocks)[block_of(target)]
    far = (block_of(target) + blocks // 2) % blocks
    return jnp.where((block_of(source) == near) | (block_of(source) == far), factor * entries, entries)


def block_levels(key, extent, cuts, least, high):
    def one(dim, parts):
        draws = jax.random.uniform(jax.random.fold_in(jax.random.fold_in(key, 6), dim), (parts,), jnp.float32, least / len(cuts), high / len(cuts))
        return jnp.repeat(jnp.exp(draws), extent[dim] // parts).reshape((-1,) + (1,) * (len(extent) - dim - 1))

    loudness = one(*cuts[0])
    for cut in cuts[1:]:
        loudness = loudness * one(*cut)
    return loudness


def normal_values(key, extent, scale, reach, cuts=(), kind=jnp.bfloat16):
    result = scale * jax.random.normal(key, extent, jnp.float32)
    if cuts:
        result = result * block_levels(key, extent, cuts, -0.22, 0.18)
    return jnp.clip(result, -reach, reach).astype(kind)


def gaussian_with(rng, extent, deviation, limit, cuts, heavy, held_as=jnp.bfloat16):
    values = deviation * jax.random.normal(rng, extent, jnp.float32)
    if cuts:
        values = values * block_levels(rng, extent, cuts, -0.22, 0.18)
    return jnp.clip(strengthened(values, jax.random.fold_in(rng, 3), *heavy), -limit, limit).astype(held_as)


def setup_inputs(seed: int = 0) -> dict:
    streams_of = jax.random.split(jax.random.key(seed), 9)
    return {
        "prompt_hidden": gaussian_with(streams_of[0], (GROUPS, PROMPT, D), 1.0, 6.0, ((0, 8), (1, 4)), (0, 2, 8, 2.0)),
        "kv_weight": normal_values(streams_of[1], (2 * KVW, D), D ** -0.5, 0.09375, ((0, 4),)),
        "queries": draw_queries(jax.random.fold_in(streams_of[8], 71), 0),
        "resp_keys": draw_resp_keys(jax.random.fold_in(streams_of[8], 71), 0),
        "resp_values": normal_values(streams_of[4], (GROUPS, TOK_RESP, KVW), 1.0, 6.0, ((0, 8), (1, 4))),
        "upstream": gaussian_with(streams_of[5], (GROUPS, TOK_RESP, QW), 1.0, 6.0, ((0, 8), (1, 4)), (1, 2, 4, 2.0)),
        "signs": place_ends(jax.random.randint(streams_of[6], (GROUPS, TOK_RESP), -1, 2), jax.random.fold_in(streams_of[6], 1), -1, 1).astype(jnp.int32),
        "lengths": place_ends(jax.random.randint(streams_of[7], (GROUPS, RESPONSES), R_DEV // 2, R_DEV + 1), jax.random.fold_in(streams_of[7], 1), R_DEV // 2, R_DEV).astype(jnp.int32),
    }


def attend(queries, cotangent, own_keys, own_values, prompt_keys, prompt_values):
    seq_len = queries.shape[0]
    per_head = HEADS // KV_HEADS
    scaling = 1.0 / math.sqrt(HEAD)
    query_full = queries.astype(jnp.float32).reshape(seq_len, KV_HEADS, per_head, HEAD)
    cotangent_full = cotangent.astype(jnp.float32).reshape(seq_len, KV_HEADS, per_head, HEAD)
    key_own = own_keys.astype(jnp.float32).reshape(seq_len, KV_HEADS, HEAD)
    value_own = own_values.astype(jnp.float32).reshape(seq_len, KV_HEADS, HEAD)
    key_prompt = prompt_keys.astype(jnp.float32).reshape(-1, KV_HEADS, HEAD)
    value_prompt = prompt_values.astype(jnp.float32).reshape(-1, KV_HEADS, HEAD)
    prompt_scores = jnp.einsum('rgqd,pgd->gqrp', query_full, key_prompt) * scaling
    own_scores = jnp.einsum('rgqd,sgd->gqrs', query_full, key_own) * scaling
    rows_index = jnp.arange(seq_len, dtype=jnp.int32)
    causal = rows_index[:, None] >= rows_index[None, :]
    own_scores = jnp.where(causal, own_scores, -jnp.inf)
    highest = jnp.maximum(lax.optimization_barrier(jnp.max(prompt_scores, axis=-1)), lax.optimization_barrier(jnp.max(own_scores, axis=-1)))[..., None]
    prompt_exp = jnp.exp(prompt_scores - highest)
    own_exp = jnp.exp(own_scores - highest)
    denominator = (lax.optimization_barrier(jnp.sum(prompt_exp, axis=-1)) + lax.optimization_barrier(jnp.sum(own_exp, axis=-1)))[..., None]
    prompt_probs = prompt_exp / denominator
    own_probs = own_exp / denominator
    prompt_half = prompt_probs.astype(jnp.bfloat16).astype(jnp.float32)
    own_half = own_probs.astype(jnp.bfloat16).astype(jnp.float32)
    mixed = jnp.einsum('gqrp,pgd->gqrd', prompt_half, value_prompt) + jnp.einsum('gqrs,sgd->gqrd', own_half, value_own)
    delta = jnp.einsum('gqrd,rgqd->gqr', mixed, cotangent_full)[..., None]
    prompt_dots = jnp.einsum('rgqd,pgd->gqrp', cotangent_full, value_prompt)
    own_dots = jnp.einsum('rgqd,sgd->gqrs', cotangent_full, value_own)
    prompt_sgrad = (prompt_probs * (prompt_dots - delta)).astype(jnp.bfloat16).astype(jnp.float32)
    own_sgrad = (own_probs * (own_dots - delta)).astype(jnp.bfloat16).astype(jnp.float32)
    key_terms = jnp.einsum('gqrp,rgqd->pgd', prompt_sgrad, query_full) * scaling
    value_terms = jnp.einsum('gqrp,rgqd->pgd', prompt_half, cotangent_full)
    key_grads = jnp.einsum('gqrs,rgqd->sgd', own_sgrad, query_full) * scaling
    value_grads = jnp.einsum('gqrs,rgqd->sgd', own_half, cotangent_full)
    key_width = KV_HEADS * HEAD
    return (key_terms.reshape(-1, key_width), value_terms.reshape(-1, key_width), key_grads.reshape(seq_len, key_width).astype(jnp.bfloat16), value_grads.reshape(seq_len, key_width).astype(jnp.bfloat16))

def reference(prompt_hidden, kv_weight, queries, resp_keys, resp_values, upstream, signs, lengths):
    key_width = KV_HEADS * HEAD
    positions = jnp.arange(R_DEV, dtype=jnp.int32)

    def per_group(carry_sum, inputs):
        hidden_rows, group_queries, group_keys, group_values, group_upstream, group_signs, group_lengths = inputs
        projected = jnp.dot(hidden_rows, kv_weight.T, preferred_element_type=jnp.float32).astype(jnp.bfloat16)
        prompt_keys = projected[:, :key_width]
        prompt_values = projected[:, key_width:]

        def per_response(pieces):
            resp_query, resp_key, resp_value, resp_upstream, resp_sign, resp_length = pieces
            live_rows = (positions < resp_length).astype(jnp.int32)
            weights = (resp_sign * live_rows).astype(jnp.bfloat16)
            cotangent = resp_upstream * weights[:, None]
            return attend(resp_query, cotangent, resp_key, resp_value, prompt_keys, prompt_values)
        key_terms, value_terms, key_grads, value_grads = lax.map(per_response, (group_queries.reshape(RESPONSES, R_DEV, -1), group_keys.reshape(RESPONSES, R_DEV, -1), group_values.reshape(RESPONSES, R_DEV, -1), group_upstream.reshape(RESPONSES, R_DEV, -1), group_signs.reshape(RESPONSES, R_DEV), group_lengths))
        prompt_grad = jnp.concatenate([lax.optimization_barrier(jnp.sum(key_terms, axis=0)), lax.optimization_barrier(jnp.sum(value_terms, axis=0))], axis=1)
        grad_half = prompt_grad.astype(jnp.bfloat16)
        weight_terms = jnp.dot(grad_half.T, hidden_rows, preferred_element_type=jnp.float32)
        return (carry_sum + weight_terms, (key_grads.reshape(TOK_RESP, key_width), value_grads.reshape(TOK_RESP, key_width)))
    initial = jnp.zeros((2 * key_width, D), jnp.float32)
    grad_weight, outputs = lax.scan(per_group, initial, (prompt_hidden, queries, resp_keys, resp_values, upstream, signs, lengths))
    return (outputs[0], outputs[1], grad_weight)
```

```python
import functools
import math

import jax
import jax.numpy as jnp
from jax import lax
from jax.experimental import pallas as pl
from jax.experimental.pallas import tpu as pltpu
from jax.sharding import PartitionSpec as P

HEADS = 32
KV_HEADS = 8
HEAD = 128
PER_HEAD = HEADS // KV_HEADS
SCALING = 1.0 / math.sqrt(HEAD)
LOG2_SCALE = SCALING * math.log2(math.e)


def dot(left, right, left_dim, right_dim):
    return lax.dot_general(
        left, right, (((left_dim,), (right_dim,)), ((), ())), preferred_element_type=jnp.float32
    )


def partner_of(index, step, count):
    if count & (count - 1) == 0:
        return index ^ step
    return (index + step) % count


def sender_to(index, step, count):
    if count & (count - 1) == 0:
        return index ^ step
    return lax.rem(index - step + count, count)


def stacked(ref, head):
    first = head * PER_HEAD
    return jnp.concatenate(
        [ref[0, :, (first + i) * HEAD : (first + i + 1) * HEAD] for i in range(PER_HEAD)], axis=0
    )


def own_kernel(q_ref, u_ref, k_ref, v_ref, exp_ref, dots_ref, stats_ref):
    seq = q_ref.shape[1]
    causal = lax.broadcasted_iota(jnp.int32, (seq, seq), 0) <= lax.broadcasted_iota(
        jnp.int32, (seq, seq), 1
    )
    for j in range(KV_HEADS):
        keys = k_ref[0, :, j * HEAD : (j + 1) * HEAD]
        values = v_ref[0, :, j * HEAD : (j + 1) * HEAD]
        for h in range(j * PER_HEAD, (j + 1) * PER_HEAD):
            cols = slice(h * HEAD, (h + 1) * HEAD)
            at = slice(h * seq, (h + 1) * seq)
            scores = jnp.where(causal, dot(keys, q_ref[0, :, cols], 1, 1), -jnp.inf)
            highest = jnp.max(scores, axis=0, keepdims=True)
            weight = jnp.exp2((scores - highest) * LOG2_SCALE)
            dots = dot(values, u_ref[0, :, cols], 1, 1)
            exp_ref[:, at] = weight
            dots_ref[:, at] = dots
            stats_ref[0:1, at] = highest
            stats_ref[1:2, at] = jnp.sum(weight, axis=0, keepdims=True)
            stats_ref[2:3, at] = jnp.sum(weight * dots, axis=0, keepdims=True)


def project_kernel(count, *refs):
    blocks, w_ref = refs[:count], refs[count]
    kv_ref, hidden_ref = refs[count + 1 :]
    me = lax.axis_index("resp")
    for step in range(count):
        hidden_ref[sender_to(me, step, count)] = blocks[step][0]
    hidden = hidden_ref[...].reshape(-1, hidden_ref.shape[-1])
    kv_ref[...] = dot(hidden, w_ref[...], 1, 1).astype(jnp.bfloat16)


def spread_kernel(chips, hidden_ref, *outs):
    me = lax.axis_index("group")
    chip, core = me // 2, lax.rem(me, 2)
    width = outs[0].shape[-1]
    for step in range(chips):
        target = partner_of(chip, step, chips)
        for side in range(2):
            group = 2 * target + (core if side == 0 else 1 - core)
            start = pl.multiple_of(group * width, width)
            outs[step][side] = hidden_ref[:, :, pl.ds(start, width)].reshape(
                outs[step].shape[1:]
            )


def prompt_kernel(count, q_ref, u_ref, signs_ref, lengths_ref, stats_ref, *refs):
    blocks = refs[:count]
    scale_ref = refs[count]
    terms_refs = refs[count + 1 : 2 * count + 1]
    kv_ref, terms_ref = refs[2 * count + 1 :]
    me = lax.axis_index("resp")
    seq = q_ref.shape[1]
    features = blocks[0].shape[1]
    for step in range(count):
        kv_ref[sender_to(me, step, count)] = blocks[step][...]

    def prompt_of(first):
        if features >= HEAD:
            at = first % features
            return kv_ref[first // features, :, at : at + HEAD]
        return jnp.concatenate(
            [kv_ref[(first + i) // features] for i in range(0, HEAD, features)], axis=1
        )

    def put(first, value):
        if features >= HEAD:
            at = first % features
            terms_ref[first // features, :, at : at + HEAD] = value
        else:
            for i in range(0, HEAD, features):
                terms_ref[(first + i) // features] = value[:, i : i + features]

    live = lax.broadcasted_iota(jnp.int32, (1, seq), 1) < lengths_ref[0, 0]
    weights = jnp.where(live, signs_ref[...], 0).astype(jnp.float32)
    weights = jnp.concatenate([weights] * PER_HEAD, axis=1)
    for j in range(KV_HEADS):
        at = slice(j * PER_HEAD * seq, (j + 1) * PER_HEAD * seq)
        queries, upstream = stacked(q_ref, j), stacked(u_ref, j)
        scores = dot(prompt_of(j * HEAD), queries, 1, 1)
        dots = dot(prompt_of((KV_HEADS + j) * HEAD), upstream, 1, 1)
        own_highest = stats_ref[0:1, at]
        highest = jnp.maximum(own_highest, jnp.max(scores, axis=0, keepdims=True))
        own_factor = jnp.exp2((own_highest - highest) * LOG2_SCALE)
        weight = jnp.exp2((scores - highest) * LOG2_SCALE)
        total = stats_ref[1:2, at] * own_factor + jnp.sum(weight, axis=0, keepdims=True)
        mixed = stats_ref[2:3, at] * own_factor + jnp.sum(weight * dots, axis=0, keepdims=True)
        inverse = 1.0 / total
        delta = mixed * inverse
        factor = weights * inverse
        probs = weight * factor
        grads = probs * (dots - delta)
        scale_ref[0:1, at] = own_factor * factor
        scale_ref[1:2, at] = delta
        put(j * HEAD, dot(grads.astype(jnp.bfloat16), queries, 1, 0) * SCALING)
        put((KV_HEADS + j) * HEAD, dot(probs.astype(jnp.bfloat16), upstream, 1, 0))
    for step in range(count):
        terms_refs[step][...] = terms_ref[partner_of(me, step, count)].astype(jnp.bfloat16)


def own_grad_kernel(q_ref, u_ref, exp_ref, dots_ref, scale_ref, gk_ref, gv_ref):
    seq = q_ref.shape[1]
    for j in range(KV_HEADS):
        probs, grads = [], []
        for h in range(j * PER_HEAD, (j + 1) * PER_HEAD):
            at = slice(h * seq, (h + 1) * seq)
            prob = exp_ref[:, at] * scale_ref[0:1, at]
            grad = prob * (dots_ref[:, at] - scale_ref[1:2, at])
            probs.append(prob.astype(jnp.bfloat16))
            grads.append(grad.astype(jnp.bfloat16))
        cols = slice(j * HEAD, (j + 1) * HEAD)
        keys = dot(jnp.concatenate(grads, axis=1), stacked(q_ref, j), 1, 0) * SCALING
        values = dot(jnp.concatenate(probs, axis=1), stacked(u_ref, j), 1, 0)
        gk_ref[0, :, cols] = keys.astype(jnp.bfloat16)
        gv_ref[0, :, cols] = values.astype(jnp.bfloat16)


def sum_kernel(*refs):
    total = refs[0][...].astype(jnp.float32)
    for ref in refs[1:-1]:
        total = total + ref[...].astype(jnp.float32)
    refs[-1][...] = total.astype(jnp.bfloat16)


def weight_kernel(count, *refs):
    left = jnp.concatenate([ref[...] for ref in refs[:count]], axis=0)
    sides = [0] * (count // 2) + [1] * (count // 2)
    right = jnp.concatenate(
        [ref[side] for ref, side in zip(refs[count : 2 * count], sides)], axis=0
    )
    refs[2 * count][...] = dot(left, right, 0, 0)


def call(kernel, outs, inputs, scratch=(), smem=(), flops=0, limit=24):
    specs = [
        pl.BlockSpec(memory_space=pltpu.SMEM if i in smem else pltpu.VMEM)
        for i in range(len(inputs))
    ]
    size = sum(x.size * x.dtype.itemsize for x in list(inputs) + list(outs))
    return pl.pallas_call(
        kernel,
        out_shape=tuple(outs),
        in_specs=specs,
        out_specs=tuple(pl.BlockSpec(memory_space=pltpu.VMEM) for _ in outs),
        scratch_shapes=list(scratch),
        cost_estimate=pl.CostEstimate(flops=flops, bytes_accessed=size, transcendentals=0),
        compiler_params=pltpu.CompilerParams(vmem_limit_bytes=limit << 20),
    )(*inputs)


def shape(dims, dtype):
    return jax.ShapeDtypeStruct(tuple(dims), dtype)


def per_device(
    resps, groups, prompt_hidden, kv_weight, queries, resp_keys, resp_values, upstream, signs, lengths
):
    chips = groups // 2

    def over_resp(value, step):
        pairs = [(i, partner_of(i, step, resps)) for i in range(resps)]
        return lax.ppermute(value, "resp", pairs)

    def over_chips(value, step):
        pairs = [(i, 2 * partner_of(i // 2, step, chips) + i % 2) for i in range(groups)]
        return lax.ppermute(value, "group", pairs)

    def swap(value):
        return lax.ppermute(value, "group", [(i, i ^ 1) for i in range(groups)])

    seq = queries.shape[1]
    rows, width = prompt_hidden.shape[1:]
    features = kv_weight.shape[0]
    prompt = rows * resps
    unit = 2 * seq * seq * HEAD * HEADS
    bf16, f32 = jnp.bfloat16, jnp.float32

    hidden_blocks = [prompt_hidden] + [over_resp(prompt_hidden, s) for s in range(1, resps)]
    exps, dots, stats = call(
        own_kernel,
        [shape((seq, HEADS * seq), f32), shape((seq, HEADS * seq), f32), shape((8, HEADS * seq), f32)],
        [queries, upstream, resp_keys, resp_values],
        flops=2 * unit,
    )
    prompt_kv, hidden = call(
        functools.partial(project_kernel, resps),
        [shape((prompt, features), bf16), shape((resps, rows, width), bf16)],
        hidden_blocks + [kv_weight],
        flops=2 * prompt * features * width,
    )
    kv_blocks = [prompt_kv] + [over_resp(prompt_kv, s) for s in range(1, resps)]
    columns = width // groups
    spread = call(
        functools.partial(spread_kernel, chips),
        [shape((2, prompt, columns), bf16)] * chips,
        [hidden],
    )
    hidden_columns = [spread[0]] + [over_chips(spread[s], s) for s in range(1, chips)]
    hidden_columns = hidden_columns + [swap(x) for x in hidden_columns]
    outs = call(
        functools.partial(prompt_kernel, resps),
        [shape((8, HEADS * seq), f32)] + [shape((prompt, features), bf16)] * resps,
        [queries, upstream, signs, lengths, stats] + kv_blocks,
        scratch=[pltpu.VMEM((resps, prompt, features), bf16), pltpu.VMEM((resps, prompt, features), f32)],
        smem=(3,),
        flops=unit,
    )
    scale, terms = outs[0], outs[1:]
    terms = [terms[0]] + [over_resp(terms[s], s) for s in range(1, resps)]
    grad_keys, grad_values = call(
        own_grad_kernel,
        [shape(resp_keys.shape, bf16), shape(resp_values.shape, bf16)],
        [queries, upstream, exps, dots, scale],
        flops=2 * unit,
    )
    (prompt_grad,) = call(sum_kernel, [shape((prompt, features), bf16)], terms)
    grad_columns = [prompt_grad] + [over_chips(prompt_grad, s) for s in range(1, chips)]
    grad_columns = grad_columns + [swap(x) for x in grad_columns]
    (grad_weight,) = call(
        functools.partial(weight_kernel, groups),
        [shape((features, columns), f32)],
        grad_columns + hidden_columns,
        flops=2 * groups * prompt * features * columns,
    )
    return (grad_keys, grad_values, grad_weight)


def solution(mesh):
    placed = (
        P("group", "resp", None),
        P("resp", None),
        P("group", "resp", None),
        P("group", "resp", None),
        P("group", "resp", None),
        P("group", "resp", None),
        P("group", "resp"),
        P("group", "resp"),
    )
    return jax.shard_map(
        functools.partial(per_device, mesh.shape["resp"], mesh.shape["group"]),
        mesh=mesh,
        in_specs=placed,
        out_specs=(P("group", "resp", None), P("group", "resp", None), P("resp", "group")),
        check_vma=False,
    )
```

```python
import functools
import math

import jax
import jax.numpy as jnp
from jax import lax
from jax.experimental import pallas as pl
from jax.experimental.pallas import tpu as pltpu
from jax.sharding import PartitionSpec as P


HEADS = 32
KV_HEADS = 8
HEAD = 128
PER_HEAD = HEADS // KV_HEADS
SCALING = 1.0 / math.sqrt(HEAD)
LOG2_SCALE = SCALING * math.log2(math.e)


def dot(left, right, left_dim, right_dim):
    return lax.dot_general(
        left, right, (((left_dim,), (right_dim,)), ((), ())), preferred_element_type=jnp.float32
    )


def partner_of(index, step, count):
    if count & (count - 1) == 0:
        return index ^ step
    return (index + step) % count


def sender_to(index, step, count):
    if count & (count - 1) == 0:
        return index ^ step
    return lax.rem(index - step + count, count)


def stacked(ref, start):
    return jnp.concatenate(
        [ref[0, :, pl.ds(start + i * HEAD, HEAD)] for i in range(PER_HEAD)], axis=0
    )


def mask_kernel(mask_ref):
    later = lax.broadcasted_iota(jnp.int32, mask_ref.shape, 0) > lax.broadcasted_iota(
        jnp.int32, mask_ref.shape, 1
    )
    mask_ref[...] = jnp.where(later, -jnp.inf, 0.0)


def own_kernel(
    mask_ref, q_ref, u_ref, k_ref, v_ref, signs_ref, lengths_ref, exp_ref, dots_ref, stats_ref
):
    seq = q_ref.shape[1]
    live = lax.broadcasted_iota(jnp.int32, signs_ref.shape, 1) < lengths_ref[...]
    row_weights = jnp.where(live, signs_ref[...], 0).astype(jnp.float32)
    for j in range(KV_HEADS):
        keys = k_ref[0, :, j * HEAD : (j + 1) * HEAD]
        values = v_ref[0, :, j * HEAD : (j + 1) * HEAD]
        for h in range(j * PER_HEAD, (j + 1) * PER_HEAD):
            cols = slice(h * HEAD, (h + 1) * HEAD)
            at = slice(h * seq, (h + 1) * seq)
            scores = dot(keys, q_ref[0, :, cols], 1, 1) + mask_ref[...]
            highest = jnp.max(scores, axis=0, keepdims=True)
            weight = jnp.exp2((scores - highest) * LOG2_SCALE)
            dots = dot(values, u_ref[0, :, cols], 1, 1)
            exp_ref[:, at] = weight
            dots_ref[:, at] = dots
            stats_ref[0:1, at] = highest
            stats_ref[1:2, at] = jnp.sum(weight, axis=0, keepdims=True)
            stats_ref[2:3, at] = jnp.sum(weight * dots, axis=0, keepdims=True)
            stats_ref[3:4, at] = row_weights


def project_kernel(count, *refs):
    blocks, w_ref = refs[:count], refs[count]
    kv_ref, hidden_ref = refs[count + 1 :]
    me = lax.axis_index("resp")
    for step in range(count):
        hidden_ref[sender_to(me, step, count)] = blocks[step][0]
    hidden = hidden_ref[...].reshape(-1, hidden_ref.shape[-1])
    kv_ref[...] = dot(hidden, w_ref[...], 1, 1).astype(jnp.bfloat16)


def spread_kernel(chips, mine_ref, partner_ref, *outs):
    me = lax.axis_index("group")
    chip, core = me // 2, lax.rem(me, 2)
    width = outs[0].shape[-1]
    for step in range(chips):
        group = 2 * partner_of(chip, step, chips) + core
        at = pl.ds(pl.multiple_of(group * width, width), width)
        for side, ref in enumerate((mine_ref, partner_ref)):
            outs[step][side] = ref[:, :, at].reshape(outs[step].shape[1:])


def prompt_head(at, queries, upstream, keys, values, stats_ref):
    scores = dot(keys, queries, 1, 1)
    dots = dot(values, upstream, 1, 1)
    own_highest = stats_ref[0:1, at]
    highest = jnp.maximum(own_highest, jnp.max(scores, axis=0, keepdims=True))
    own_factor = jnp.exp2((own_highest - highest) * LOG2_SCALE)
    weight = jnp.exp2((scores - highest) * LOG2_SCALE)
    total = stats_ref[1:2, at] * own_factor + jnp.sum(weight, axis=0, keepdims=True)
    mixed = stats_ref[2:3, at] * own_factor + jnp.sum(weight * dots, axis=0, keepdims=True)
    inverse = 1.0 / total
    delta = mixed * inverse
    factor = stats_ref[3:4, at] * inverse
    probs = weight * factor
    grads = probs * (dots - delta)
    key_terms = dot(grads.astype(jnp.bfloat16), queries, 1, 0) * SCALING
    value_terms = dot(probs.astype(jnp.bfloat16), upstream, 1, 0)
    return key_terms, value_terms, own_factor * factor, delta


def pair_kernel(
    count, step, q_ref, u_ref, stats_ref, near_ref, far_ref,
    scale_ref, near_terms_ref, far_terms_ref, kv_ref, terms_ref,
):
    seq = q_ref.shape[1]
    heads = near_ref.shape[1] // HEAD
    index = lax.axis_index("resp") ^ step
    pair, side = lax.rem(index, count // 2), index // (count // 2)
    kv_ref[side] = near_ref[...]
    kv_ref[1 - side] = far_ref[...]
    size = PER_HEAD * HEAD
    for i in range(heads):
        start = pl.multiple_of((pair * heads + i) * size, size)
        queries, upstream = stacked(q_ref, start), stacked(u_ref, start)
        at = slice(i * HEAD, (i + 1) * HEAD)
        stats_at = pl.ds(pl.multiple_of((pair * heads + i) * PER_HEAD * seq, PER_HEAD * seq), PER_HEAD * seq)
        key_terms, value_terms, factor, delta = prompt_head(
            stats_at, queries, upstream, kv_ref[0, :, at], kv_ref[1, :, at], stats_ref
        )
        here = slice(i * PER_HEAD * seq, (i + 1) * PER_HEAD * seq)
        scale_ref[0:1, here] = factor
        scale_ref[1:2, here] = delta
        terms_ref[0, :, at] = key_terms.astype(jnp.bfloat16)
        terms_ref[1, :, at] = value_terms.astype(jnp.bfloat16)
    near_terms_ref[...] = terms_ref[side]
    far_terms_ref[...] = terms_ref[1 - side]


def prompt_kernel(count, q_ref, u_ref, stats_ref, *refs):
    blocks = refs[:count]
    scale_ref = refs[count]
    terms_refs = refs[count + 1 : 2 * count + 1]
    kv_ref, terms_ref = refs[2 * count + 1 :]
    me = lax.axis_index("resp")
    seq = q_ref.shape[1]
    features = blocks[0].shape[1]
    for step in range(count):
        kv_ref[sender_to(me, step, count)] = blocks[step][...]

    def prompt_of(first):
        if features >= HEAD:
            at = first % features
            return kv_ref[first // features, :, at : at + HEAD]
        return jnp.concatenate(
            [kv_ref[(first + i) // features] for i in range(0, HEAD, features)], axis=1
        )

    def put(first, value):
        if features >= HEAD:
            at = first % features
            terms_ref[first // features, :, at : at + HEAD] = value
        else:
            for i in range(0, HEAD, features):
                terms_ref[(first + i) // features] = value[:, i : i + features]

    for j in range(KV_HEADS):
        at = slice(j * PER_HEAD * seq, (j + 1) * PER_HEAD * seq)
        start = j * PER_HEAD * HEAD
        key_terms, value_terms, factor, delta = prompt_head(
            at, stacked(q_ref, start), stacked(u_ref, start),
            prompt_of(j * HEAD), prompt_of((KV_HEADS + j) * HEAD), stats_ref,
        )
        scale_ref[0:1, at] = factor
        scale_ref[1:2, at] = delta
        put(j * HEAD, key_terms)
        put((KV_HEADS + j) * HEAD, value_terms)
    for step in range(count):
        terms_refs[step][...] = terms_ref[partner_of(me, step, count)].astype(jnp.bfloat16)


def own_grad_kernel(steps, count, q_ref, u_ref, exp_ref, dots_ref, *refs):
    seq = q_ref.shape[1]
    gk_ref, gv_ref = refs[len(steps) :]
    for step, scale_ref in zip(steps, refs):
        heads = scale_ref.shape[1] // (PER_HEAD * seq)
        first = 0
        if len(steps) > 1:
            first = lax.rem(lax.axis_index("resp") ^ step, count // 2) * heads
        for j in range(heads):
            probs, grads = [], []
            for h in range(PER_HEAD):
                here = slice((j * PER_HEAD + h) * seq, (j * PER_HEAD + h + 1) * seq)
                start = ((first + j) * PER_HEAD + h) * seq
                at = pl.ds(start if len(steps) == 1 else pl.multiple_of(start, seq), seq)
                prob = exp_ref[:, at] * scale_ref[0:1, here]
                grad = prob * (dots_ref[:, at] - scale_ref[1:2, here])
                probs.append(prob.astype(jnp.bfloat16))
                grads.append(grad.astype(jnp.bfloat16))
            start, column = (first + j) * PER_HEAD * HEAD, (first + j) * HEAD
            if len(steps) > 1:
                start, column = pl.multiple_of(start, HEAD), pl.multiple_of(column, HEAD)
            cols = pl.ds(column, HEAD)
            keys = dot(jnp.concatenate(grads, axis=1), stacked(q_ref, start), 1, 0) * SCALING
            values = dot(jnp.concatenate(probs, axis=1), stacked(u_ref, start), 1, 0)
            gk_ref[0, :, cols] = keys.astype(jnp.bfloat16)
            gv_ref[0, :, cols] = values.astype(jnp.bfloat16)


def sum_kernel(*refs):
    total = refs[0][...].astype(jnp.float32)
    for ref in refs[1:-1]:
        total = total + ref[...].astype(jnp.float32)
    refs[-1][...] = total.astype(jnp.bfloat16)


def weight_kernel(chips, *refs):
    grads, columns, out_ref = refs[: 2 * chips], refs[2 * chips : 3 * chips], refs[3 * chips]
    left = jnp.concatenate([ref[...] for ref in grads], axis=0)
    right = jnp.concatenate([ref[side] for side in range(2) for ref in columns], axis=0)
    out_ref[...] = dot(left, right, 0, 0)


def call(kernel, outs, inputs, scratch=(), kinds={}, flops=0, limit=24):
    size = sum(x.size * x.dtype.itemsize for x in list(inputs) + list(outs))
    return pl.pallas_call(
        kernel,
        out_shape=tuple(outs),
        in_specs=[pl.BlockSpec(memory_space=kinds.get(i, pltpu.VMEM)) for i in range(len(inputs))],
        out_specs=tuple(pl.BlockSpec(memory_space=pltpu.VMEM) for _ in outs),
        scratch_shapes=list(scratch),
        cost_estimate=pl.CostEstimate(flops=flops, bytes_accessed=size, transcendentals=0),
        compiler_params=pltpu.CompilerParams(vmem_limit_bytes=limit << 20),
    )(*inputs)


def shape(dims, dtype):
    return jax.ShapeDtypeStruct(tuple(dims), dtype)


def per_device(
    resps, groups, prompt_hidden, kv_weight, queries, resp_keys, resp_values, upstream, signs, lengths
):
    chips = groups // 2

    def over_resp(value, step):
        pairs = [(i, partner_of(i, step, resps)) for i in range(resps)]
        return lax.ppermute(value, "resp", pairs)

    def over_chips(value, step):
        pairs = [(i, 2 * partner_of(i // 2, step, chips) + i % 2) for i in range(groups)]
        return lax.ppermute(value, "group", pairs)

    def swap(value):
        return lax.ppermute(value, "group", [(i, i ^ 1) for i in range(groups)])

    seq = queries.shape[1]
    rows, width = prompt_hidden.shape[1:]
    features = kv_weight.shape[0]
    prompt = rows * resps
    unit = 2 * seq * seq * HEAD * HEADS
    bf16, f32 = jnp.bfloat16, jnp.float32
    block = shape((prompt, features), bf16)

    (mask,) = call(mask_kernel, [shape((seq, seq), f32)], [], flops=MASK_FLOPS)
    hidden_blocks = [prompt_hidden] + [over_resp(prompt_hidden, s) for s in range(1, resps)]
    wide = shape((seq, HEADS * seq), f32)
    exps, dots, stats = call(
        own_kernel,
        [wide, wide, shape((8, HEADS * seq), f32)],
        [mask, queries, upstream, resp_keys, resp_values, signs, lengths],
        flops=OWN_FLOPS,
    )
    prompt_kv, hidden = call(
        functools.partial(project_kernel, resps),
        [block, shape((resps, rows, width), bf16)],
        hidden_blocks + [kv_weight],
        flops=2 * prompt * features * width,
    )
    kv_blocks = [prompt_kv] + [over_resp(prompt_kv, s) for s in range(1, resps)]
    terms = [None] * resps
    if paired(resps, features):
        half = resps // 2
        steps, scales = tuple(range(half)), []
        for s in steps:
            scale, terms[s], terms[s + half] = call(
                functools.partial(pair_kernel, resps, s),
                [shape((8, features // HEAD * PER_HEAD * seq), f32), block, block],
                [queries, upstream, stats, kv_blocks[s], kv_blocks[s + half]],
                scratch=[pltpu.VMEM((2, prompt, features), bf16)] * 2,
                flops=unit // half,
            )
            scales.append(scale)
    else:
        steps = (0,)
        scale, *terms = call(
            functools.partial(prompt_kernel, resps),
            [shape((8, HEADS * seq), f32)] + [block] * resps,
            [queries, upstream, stats] + kv_blocks,
            scratch=[
                pltpu.VMEM((resps, prompt, features), bf16),
                pltpu.VMEM((resps, prompt, features), f32),
            ],
            flops=unit,
        )
        scales = [scale]
    terms = [terms[0]] + [over_resp(terms[s], s) for s in range(1, resps)]
    columns = width // groups
    spread = call(
        functools.partial(spread_kernel, chips),
        [shape((2, prompt, columns), bf16)] * chips,
        [hidden, swap(hidden)],
    )
    hidden_columns = [spread[0]] + [over_chips(spread[s], s) for s in range(1, chips)]
    (prompt_grad,) = call(sum_kernel, [block], terms)
    grad_columns = [prompt_grad] + [over_chips(prompt_grad, s) for s in range(1, chips)]
    grad_columns = grad_columns + [swap(x) for x in grad_columns]
    grad_keys, grad_values = call(
        functools.partial(own_grad_kernel, steps, resps),
        [shape(resp_keys.shape, bf16), shape(resp_values.shape, bf16)],
        [queries, upstream, exps, dots] + scales,
        flops=2 * unit,
    )
    (grad_weight,) = call(
        functools.partial(weight_kernel, chips),
        [shape((features, columns), f32)],
        grad_columns + hidden_columns,
        flops=2 * groups * prompt * features * columns,
    )
    return (grad_keys, grad_values, grad_weight)


def paired(resps, features):
    return resps > 1 and resps & (resps - 1) == 0 and features % HEAD == 0


MASK_FLOPS = OWN_FLOPS = 20_000_000_000


def solution(mesh):
    placed = (
        P("group", "resp", None),
        P("resp", None),
        P("group", "resp", None),
        P("group", "resp", None),
        P("group", "resp", None),
        P("group", "resp", None),
        P("group", "resp"),
        P("group", "resp"),
    )

    def body(*args):
        return per_device(mesh.shape["resp"], mesh.shape["group"], *args)

    return jax.shard_map(
        body,
        mesh=mesh,
        in_specs=placed,
        out_specs=(P("group", "resp", None), P("group", "resp", None), P("resp", "group")),
        check_vma=False,
    )
```

```python
import functools
import math

import jax
import jax.numpy as jnp
from jax import lax
from jax.experimental import pallas as pl
from jax.experimental.pallas import tpu as pltpu
from jax.sharding import PartitionSpec as P


HEADS = 32
KV_HEADS = 8
HEAD = 128
PER_HEAD = HEADS // KV_HEADS
SCALING = 1.0 / math.sqrt(HEAD)
LOG2_SCALE = SCALING * math.log2(math.e)


def dot(left, right, left_dim, right_dim):
    return lax.dot_general(
        left, right, (((left_dim,), (right_dim,)), ((), ())), preferred_element_type=jnp.float32
    )


def partner_of(index, step, count):
    if count & (count - 1) == 0:
        return index ^ step
    return (index + step) % count


def sender_to(index, step, count):
    if count & (count - 1) == 0:
        return index ^ step
    return lax.rem(index - step + count, count)


def stacked(ref, start):
    return jnp.concatenate(
        [ref[0, :, pl.ds(start + i * HEAD, HEAD)] for i in range(PER_HEAD)], axis=0
    )


def mask_kernel(mask_ref):
    later = lax.broadcasted_iota(jnp.int32, mask_ref.shape, 0) > lax.broadcasted_iota(
        jnp.int32, mask_ref.shape, 1
    )
    mask_ref[...] = jnp.where(later, -jnp.inf, 0.0)


def own_kernel(
    mask_ref, q_ref, u_ref, k_ref, v_ref, signs_ref, lengths_ref,
    qt_ref, ut_ref, exp_ref, dots_ref, stats_ref,
):
    seq = q_ref.shape[1]
    live = lax.broadcasted_iota(jnp.int32, signs_ref.shape, 1) < lengths_ref[...]
    row_weights = jnp.where(live, signs_ref[...], 0).astype(jnp.float32)
    for j in range(KV_HEADS):
        keys = k_ref[0, :, j * HEAD : (j + 1) * HEAD]
        values = v_ref[0, :, j * HEAD : (j + 1) * HEAD]
        for h in range(j * PER_HEAD, (j + 1) * PER_HEAD):
            cols = slice(h * HEAD, (h + 1) * HEAD)
            at = slice(h * seq, (h + 1) * seq)
            queries, upstream = q_ref[0, :, cols].T, u_ref[0, :, cols].T
            qt_ref[:, at], ut_ref[:, at] = queries, upstream
            scores = dot(keys, queries, 1, 0) + mask_ref[...]
            highest = jnp.max(scores, axis=0, keepdims=True)
            weight = jnp.exp2((scores - highest) * LOG2_SCALE)
            dots = dot(values, upstream, 1, 0)
            exp_ref[:, at] = weight
            dots_ref[:, at] = dots
            stats_ref[0:1, at] = highest
            stats_ref[1:2, at] = jnp.sum(weight, axis=0, keepdims=True)
            stats_ref[2:3, at] = jnp.sum(weight * dots, axis=0, keepdims=True)
            stats_ref[3:4, at] = row_weights


def turn_kernel(w_ref, out_ref):
    for start in range(0, w_ref.shape[1], HEAD):
        out_ref[start : start + HEAD] = w_ref[:, start : start + HEAD].T


def project_kernel(count, *refs):
    blocks, w_ref = refs[:count], refs[count]
    kv_ref, hidden_ref = refs[count + 1 :]
    me = lax.axis_index("resp")
    for step in range(count):
        hidden_ref[sender_to(me, step, count)] = blocks[step][0]
    hidden = hidden_ref[...].reshape(-1, hidden_ref.shape[-1])
    kv_ref[...] = dot(hidden, w_ref[...], 1, 0).astype(jnp.bfloat16)


def spread_kernel(chips, mine_ref, partner_ref, *outs):
    me = lax.axis_index("group")
    chip, core = me // 2, lax.rem(me, 2)
    width = outs[0].shape[-1]
    for step in range(chips):
        group = 2 * partner_of(chip, step, chips) + core
        at = pl.ds(pl.multiple_of(group * width, width), width)
        for side, ref in enumerate((mine_ref, partner_ref)):
            outs[step][side] = ref[:, :, at].reshape(outs[step].shape[1:])


def prompt_head(at, q_ref, u_ref, qt_ref, ut_ref, start, keys, values, stats_ref):
    scores = dot(keys, qt_ref[:, at], 1, 0)
    dots = dot(values, ut_ref[:, at], 1, 0)
    own_highest = stats_ref[0:1, at]
    highest = jnp.maximum(own_highest, jnp.max(scores, axis=0, keepdims=True))
    own_factor = jnp.exp2((own_highest - highest) * LOG2_SCALE)
    weight = jnp.exp2((scores - highest) * LOG2_SCALE)
    total = stats_ref[1:2, at] * own_factor + jnp.sum(weight, axis=0, keepdims=True)
    mixed = stats_ref[2:3, at] * own_factor + jnp.sum(weight * dots, axis=0, keepdims=True)
    inverse = 1.0 / total
    delta = mixed * inverse
    factor = stats_ref[3:4, at] * inverse
    probs = weight * factor
    grads = probs * (dots - delta)
    key_terms = dot(grads.astype(jnp.bfloat16), stacked(q_ref, start), 1, 0) * SCALING
    value_terms = dot(probs.astype(jnp.bfloat16), stacked(u_ref, start), 1, 0)
    return key_terms, value_terms, own_factor * factor, delta


def pair_kernel(
    count, step, q_ref, u_ref, qt_ref, ut_ref, stats_ref, near_ref, far_ref,
    scale_ref, near_terms_ref, far_terms_ref, kv_ref, terms_ref,
):
    seq = q_ref.shape[1]
    heads = near_ref.shape[1] // HEAD
    index = lax.axis_index("resp") ^ step
    pair, side = lax.rem(index, count // 2), index // (count // 2)
    kv_ref[side] = near_ref[...]
    kv_ref[1 - side] = far_ref[...]
    size = PER_HEAD * HEAD
    for i in range(heads):
        start = pl.multiple_of((pair * heads + i) * size, size)
        at = slice(i * HEAD, (i + 1) * HEAD)
        stats_at = pl.ds(pl.multiple_of((pair * heads + i) * PER_HEAD * seq, PER_HEAD * seq), PER_HEAD * seq)
        key_terms, value_terms, factor, delta = prompt_head(
            stats_at, q_ref, u_ref, qt_ref, ut_ref, start, kv_ref[0, :, at], kv_ref[1, :, at], stats_ref
        )
        here = slice(i * PER_HEAD * seq, (i + 1) * PER_HEAD * seq)
        scale_ref[0:1, here] = factor
        scale_ref[1:2, here] = delta
        terms_ref[0, :, at] = key_terms.astype(jnp.bfloat16)
        terms_ref[1, :, at] = value_terms.astype(jnp.bfloat16)
    near_terms_ref[...] = terms_ref[side]
    far_terms_ref[...] = terms_ref[1 - side]


def prompt_kernel(count, q_ref, u_ref, qt_ref, ut_ref, stats_ref, *refs):
    blocks = refs[:count]
    scale_ref = refs[count]
    terms_refs = refs[count + 1 : 2 * count + 1]
    kv_ref, terms_ref = refs[2 * count + 1 :]
    me = lax.axis_index("resp")
    seq = q_ref.shape[1]
    features = blocks[0].shape[1]
    for step in range(count):
        kv_ref[sender_to(me, step, count)] = blocks[step][...]

    def prompt_of(first):
        if features >= HEAD:
            at = first % features
            return kv_ref[first // features, :, at : at + HEAD]
        return jnp.concatenate(
            [kv_ref[(first + i) // features] for i in range(0, HEAD, features)], axis=1
        )

    def put(first, value):
        if features >= HEAD:
            at = first % features
            terms_ref[first // features, :, at : at + HEAD] = value
        else:
            for i in range(0, HEAD, features):
                terms_ref[(first + i) // features] = value[:, i : i + features]

    for j in range(KV_HEADS):
        at = slice(j * PER_HEAD * seq, (j + 1) * PER_HEAD * seq)
        start = j * PER_HEAD * HEAD
        key_terms, value_terms, factor, delta = prompt_head(
            at, q_ref, u_ref, qt_ref, ut_ref, start,
            prompt_of(j * HEAD), prompt_of((KV_HEADS + j) * HEAD), stats_ref,
        )
        scale_ref[0:1, at] = factor
        scale_ref[1:2, at] = delta
        put(j * HEAD, key_terms)
        put((KV_HEADS + j) * HEAD, value_terms)
    for step in range(count):
        terms_refs[step][...] = terms_ref[partner_of(me, step, count)].astype(jnp.bfloat16)


def first_head(step, count, heads):
    if heads == KV_HEADS:
        return 0
    return lax.rem(lax.axis_index("resp") ^ step, count // 2) * heads


def own_grad(step, count, q_ref, u_ref, exp_ref, dots_ref, scale_ref, out_ref):
    seq = q_ref.shape[1]
    heads = scale_ref.shape[1] // (PER_HEAD * seq)
    first = first_head(step, count, heads)
    size = PER_HEAD * HEAD
    for j in range(heads):
        probs, grads = [], []
        for h in range(PER_HEAD):
            here = slice((j * PER_HEAD + h) * seq, (j * PER_HEAD + h + 1) * seq)
            at = pl.ds(pl.multiple_of(((first + j) * PER_HEAD + h) * seq, seq), seq)
            prob = exp_ref[:, at] * scale_ref[0:1, here]
            grad = prob * (dots_ref[:, at] - scale_ref[1:2, here])
            probs.append(prob.astype(jnp.bfloat16))
            grads.append(grad.astype(jnp.bfloat16))
        start = pl.multiple_of((first + j) * size, size)
        cols = slice(j * HEAD, (j + 1) * HEAD)
        keys = dot(jnp.concatenate(grads, axis=1), stacked(q_ref, start), 1, 0) * SCALING
        values = dot(jnp.concatenate(probs, axis=1), stacked(u_ref, start), 1, 0)
        out_ref[0, :, cols] = keys.astype(jnp.bfloat16)
        out_ref[1, :, cols] = values.astype(jnp.bfloat16)


def own_grad_kernel(step, count, *refs):
    own_grad(step, count, *refs)


def last_own_grad_kernel(steps, count, q_ref, u_ref, exp_ref, dots_ref, scale_ref, *refs):
    parts, (gk_ref, gv_ref, held_ref, sems) = refs[: len(steps) - 1], refs[len(steps) - 1 :]
    copies = []

    def store(i, ref):
        heads = ref.shape[2] // HEAD
        first = first_head(steps[i], count, heads) * HEAD
        at = pl.ds(pl.multiple_of(first, HEAD), heads * HEAD)
        for side, target in enumerate((gk_ref, gv_ref)):
            copies.append(pltpu.make_async_copy(ref.at[side], target.at[0, :, at], sems.at[side, i]))
            copies[-1].start()

    for i, ref in enumerate(parts):
        store(i, ref)
    own_grad(steps[-1], count, q_ref, u_ref, exp_ref, dots_ref, scale_ref, held_ref)
    store(len(steps) - 1, held_ref)
    for copy in copies:
        copy.wait()


def sum_kernel(*refs):
    total = refs[0][...].astype(jnp.float32)
    for ref in refs[1:-1]:
        total = total + ref[...].astype(jnp.float32)
    refs[-1][...] = total.astype(jnp.bfloat16)


def weight_kernel(chips, *refs):
    grads, columns, (out_ref, held_ref, sems) = refs[: 2 * chips], refs[2 * chips : 3 * chips], refs[3 * chips :]
    right = jnp.concatenate([ref[side] for side in range(2) for ref in columns], axis=0)
    copies = []
    width = held_ref.shape[0] // sems.shape[0]
    for i in range(sems.shape[0]):
        rows = slice(i * width, (i + 1) * width)
        left = jnp.concatenate([ref[:, rows] for ref in grads], axis=0)
        held_ref[rows] = dot(left, right, 0, 0)
        copies.append(pltpu.make_async_copy(held_ref.at[rows], out_ref.at[rows], sems.at[i]))
        copies[-1].start()
    for copy in copies:
        copy.wait()


def call(kernel, outs, inputs, scratch=(), kinds={}, out_kind=pltpu.VMEM, flops=0, limit=24):
    size = sum(x.size * x.dtype.itemsize for x in list(inputs) + list(outs))
    return pl.pallas_call(
        kernel,
        out_shape=tuple(outs),
        in_specs=[pl.BlockSpec(memory_space=kinds.get(i, pltpu.VMEM)) for i in range(len(inputs))],
        out_specs=tuple(pl.BlockSpec(memory_space=out_kind) for _ in outs),
        scratch_shapes=list(scratch),
        cost_estimate=pl.CostEstimate(flops=flops, bytes_accessed=size, transcendentals=0),
        compiler_params=pltpu.CompilerParams(vmem_limit_bytes=limit << 20),
    )(*inputs)


def shape(dims, dtype):
    return jax.ShapeDtypeStruct(tuple(dims), dtype)


def per_device(
    resps, groups, prompt_hidden, kv_weight, queries, resp_keys, resp_values, upstream, signs, lengths
):
    chips = groups // 2

    def over_resp(value, step):
        pairs = [(i, partner_of(i, step, resps)) for i in range(resps)]
        return lax.ppermute(value, "resp", pairs)

    def over_chips(value, step):
        pairs = [(i, 2 * partner_of(i // 2, step, chips) + i % 2) for i in range(groups)]
        return lax.ppermute(value, "group", pairs)

    def swap(value):
        return lax.ppermute(value, "group", [(i, i ^ 1) for i in range(groups)])

    seq = queries.shape[1]
    rows, width = prompt_hidden.shape[1:]
    features = kv_weight.shape[0]
    prompt = rows * resps
    unit = 2 * seq * seq * HEAD * HEADS
    bf16, f32 = jnp.bfloat16, jnp.float32
    block = shape((prompt, features), bf16)

    (mask,) = call(mask_kernel, [shape((seq, seq), f32)], [], flops=MASK_FLOPS)
    hidden_blocks = [prompt_hidden] + [over_resp(prompt_hidden, s) for s in range(1, resps)]
    wide = shape((seq, HEADS * seq), f32)
    turned = shape((HEAD, HEADS * seq), bf16)
    queries_t, upstream_t, exps, dots, stats = call(
        own_kernel,
        [turned, turned, wide, wide, shape((8, HEADS * seq), f32)],
        [mask, queries, upstream, resp_keys, resp_values, signs, lengths],
        flops=OWN_FLOPS,
    )
    (weight_t,) = call(turn_kernel, [shape((width, features), bf16)], [kv_weight])
    prompt_kv, hidden = call(
        functools.partial(project_kernel, resps),
        [block, shape((resps, rows, width), bf16)],
        hidden_blocks + [weight_t],
        flops=2 * prompt * features * width,
    )
    kv_blocks = [prompt_kv] + [over_resp(prompt_kv, s) for s in range(1, resps)]
    terms = [None] * resps
    if paired(resps, features):
        half = resps // 2
        steps, scales = tuple(range(half)), []
        for s in steps:
            scale, terms[s], terms[s + half] = call(
                functools.partial(pair_kernel, resps, s),
                [shape((8, features // HEAD * PER_HEAD * seq), f32), block, block],
                [queries, upstream, queries_t, upstream_t, stats, kv_blocks[s], kv_blocks[s + half]],
                scratch=[pltpu.VMEM((2, prompt, features), bf16)] * 2,
                flops=unit // half,
            )
            scales.append(scale)
    else:
        steps = (0,)
        scale, *terms = call(
            functools.partial(prompt_kernel, resps),
            [shape((8, HEADS * seq), f32)] + [block] * resps,
            [queries, upstream, queries_t, upstream_t, stats] + kv_blocks,
            scratch=[
                pltpu.VMEM((resps, prompt, features), bf16),
                pltpu.VMEM((resps, prompt, features), f32),
            ],
            flops=unit,
        )
        scales = [scale]
    terms = [terms[0]] + [over_resp(terms[s], s) for s in range(1, resps)]
    columns = width // groups
    spread = call(
        functools.partial(spread_kernel, chips),
        [shape((2, prompt, columns), bf16)] * chips,
        [hidden, swap(hidden)],
    )
    hidden_columns = [spread[0]] + [over_chips(spread[s], s) for s in range(1, chips)]
    (prompt_grad,) = call(sum_kernel, [block], terms)
    grad_columns = [prompt_grad] + [over_chips(prompt_grad, s) for s in range(1, chips)]
    grad_columns = grad_columns + [swap(x) for x in grad_columns]
    halves = []
    for step, scale in zip(steps[:-1], scales):
        (own,) = call(
            functools.partial(own_grad_kernel, step, resps),
            [shape((2, seq, scale.shape[1] // (PER_HEAD * seq) * HEAD), bf16)],
            [queries, upstream, exps, dots, scale],
            flops=2 * unit // len(steps),
        )
        halves.append(own)
    grad_keys, grad_values = call(
        functools.partial(last_own_grad_kernel, steps, resps),
        [shape(resp_keys.shape, bf16), shape(resp_values.shape, bf16)],
        [queries, upstream, exps, dots, scales[-1]] + halves,
        scratch=[
            pltpu.VMEM((2, seq, scales[-1].shape[1] // (PER_HEAD * seq) * HEAD), bf16),
            pltpu.SemaphoreType.DMA((2, len(steps))),
        ],
        out_kind=pl.ANY,
        flops=2 * unit // len(steps),
    )
    (grad_weight,) = call(
        functools.partial(weight_kernel, chips),
        [shape((features, columns), f32)],
        grad_columns + hidden_columns,
        scratch=[
            pltpu.VMEM((features, columns), f32),
            pltpu.SemaphoreType.DMA((max(1, features // HEAD),)),
        ],
        out_kind=pl.ANY,
        flops=2 * groups * prompt * features * columns,
    )
    return (grad_keys, grad_values, grad_weight)


def paired(resps, features):
    return resps > 1 and resps & (resps - 1) == 0 and features % HEAD == 0


MASK_FLOPS = OWN_FLOPS = 20_000_000_000


def solution(mesh):
    placed = (
        P("group", "resp", None),
        P("resp", None),
        P("group", "resp", None),
        P("group", "resp", None),
        P("group", "resp", None),
        P("group", "resp", None),
        P("group", "resp"),
        P("group", "resp"),
    )

    def body(*args):
        return per_device(mesh.shape["resp"], mesh.shape["group"], *args)

    return jax.shard_map(
        body,
        mesh=mesh,
        in_specs=placed,
        out_specs=(P("group", "resp", None), P("group", "resp", None), P("resp", "group")),
        check_vma=False,
    )
```

```python
import functools
import math

import jax
import jax.numpy as jnp
from jax import lax
from jax.experimental import pallas as pl
from jax.experimental.pallas import tpu as pltpu
from jax.sharding import PartitionSpec as P


HEADS = 32
KV_HEADS = 8
HEAD = 128
PER_HEAD = HEADS // KV_HEADS
SCALING = 1.0 / math.sqrt(HEAD)
LOG2_SCALE = SCALING * math.log2(math.e)


def dot(left, right, left_dim, right_dim):
    return lax.dot_general(
        left, right, (((left_dim,), (right_dim,)), ((), ())), preferred_element_type=jnp.float32
    )


def partner_of(index, step, count):
    if count & (count - 1) == 0:
        return index ^ step
    return (index + step) % count


def sender_to(index, step, count):
    if count & (count - 1) == 0:
        return index ^ step
    return lax.rem(index - step + count, count)


def stacked(ref, start):
    return jnp.concatenate(
        [ref[0, :, pl.ds(start + i * HEAD, HEAD)] for i in range(PER_HEAD)], axis=0
    )


def mask_kernel(mask_ref):
    later = lax.broadcasted_iota(jnp.int32, mask_ref.shape, 0) > lax.broadcasted_iota(
        jnp.int32, mask_ref.shape, 1
    )
    mask_ref[...] = jnp.where(later, -jnp.inf, 0.0)


def rows_kernel(signs_ref, lengths_ref, out_ref):
    live = lax.broadcasted_iota(jnp.int32, signs_ref.shape, 1) < lengths_ref[...]
    weights = jnp.where(live, signs_ref[...], 0).astype(jnp.float32)
    out_ref[...] = jnp.concatenate([weights] * PER_HEAD, axis=1)


def own_kernel(
    mask_ref, q_ref, u_ref, k_ref, v_ref,
    qt_ref, ut_ref, exp_ref, dots_ref, stats_ref,
):
    seq = q_ref.shape[1]
    for j in range(KV_HEADS):
        keys = k_ref[0, :, j * HEAD : (j + 1) * HEAD]
        values = v_ref[0, :, j * HEAD : (j + 1) * HEAD]
        for h in range(j * PER_HEAD, (j + 1) * PER_HEAD):
            cols = slice(h * HEAD, (h + 1) * HEAD)
            at = slice(h * seq, (h + 1) * seq)
            queries, upstream = q_ref[0, :, cols].T, u_ref[0, :, cols].T
            qt_ref[:, at], ut_ref[:, at] = queries, upstream
            scores = dot(keys, queries, 1, 0) + mask_ref[...]
            highest = jnp.max(scores, axis=0, keepdims=True)
            weight = jnp.exp2((scores - highest) * LOG2_SCALE)
            dots = dot(values, upstream, 1, 0)
            exp_ref[:, at] = weight
            dots_ref[:, at] = dots
            stats_ref[0:1, at] = highest
            stats_ref[1:2, at] = jnp.sum(weight, axis=0, keepdims=True)
            stats_ref[2:3, at] = jnp.sum(weight * dots, axis=0, keepdims=True)


def turn_kernel(w_ref, out_ref):
    for start in range(0, w_ref.shape[1], HEAD):
        out_ref[start : start + HEAD] = w_ref[:, start : start + HEAD].T


def project_kernel(count, *refs):
    blocks, w_ref = refs[:count], refs[count]
    kv_ref, hidden_ref = refs[count + 1 :]
    me = lax.axis_index("resp")
    for step in range(count):
        hidden_ref[sender_to(me, step, count)] = blocks[step][0]
    hidden = hidden_ref[...].reshape(-1, hidden_ref.shape[-1])
    kv_ref[...] = dot(hidden, w_ref[...], 1, 0).astype(jnp.bfloat16)


def spread_kernel(chips, mine_ref, partner_ref, *outs):
    me = lax.axis_index("group")
    chip, core = me // 2, lax.rem(me, 2)
    width = outs[0].shape[-1]
    for step in range(chips):
        group = 2 * partner_of(chip, step, chips) + (core if step == 0 else 1 - core)
        at = pl.ds(pl.multiple_of(group * width, width), width)
        for side, ref in enumerate((mine_ref, partner_ref)):
            outs[step][side] = ref[:, :, at].reshape(outs[step].shape[1:])


def prompt_heads(heads, q_ref, u_ref, qt_ref, ut_ref, rows_ref, stats_ref):
    spans = []
    seq = q_ref.shape[1]
    for _, _, first in heads:
        start, at = first * HEAD, first * seq
        if not isinstance(first, int):
            start, at = pl.multiple_of(start, PER_HEAD * HEAD), pl.multiple_of(at, PER_HEAD * seq)
        spans.append((start, pl.ds(at, PER_HEAD * seq)))
    products = [
        (dot(keys, qt_ref[:, at], 1, 0), dot(values, ut_ref[:, at], 1, 0))
        for (keys, values, _), (_, at) in zip(heads, spans)
    ]
    rows = [tuple(stats_ref[i : i + 1, at] for i in range(3)) for _, at in spans]
    halves = []
    row_weights = rows_ref[...]
    for (scores, dots), (own_highest, own_total, own_mixed) in zip(products, rows):
        highest = jnp.maximum(own_highest, jnp.max(scores, axis=0, keepdims=True))
        own_factor = jnp.exp2((own_highest - highest) * LOG2_SCALE)
        weight = jnp.exp2((scores - highest) * LOG2_SCALE)
        total = own_total * own_factor + jnp.sum(weight, axis=0, keepdims=True)
        mixed = own_mixed * own_factor + jnp.sum(weight * dots, axis=0, keepdims=True)
        inverse = 1.0 / total
        delta = mixed * inverse
        factor = row_weights * inverse
        probs = weight * factor
        grads = probs * (dots - delta)
        halves.append(
            (grads.astype(jnp.bfloat16), probs.astype(jnp.bfloat16), own_factor * factor, delta)
        )
    return [
        (
            dot(grads, stacked(q_ref, start), 1, 0) * SCALING,
            dot(probs, stacked(u_ref, start), 1, 0),
            factor,
            delta,
        )
        for (grads, probs, factor, delta), (start, _) in zip(halves, spans)
    ]


def pair_kernel(
    count, step, q_ref, u_ref, qt_ref, ut_ref, rows_ref, stats_ref, near_ref, far_ref,
    scale_ref, near_terms_ref, far_terms_ref, kv_ref, terms_ref,
):
    seq = q_ref.shape[1]
    heads = near_ref.shape[1] // HEAD
    index = lax.axis_index("resp") ^ step
    pair, side = lax.rem(index, count // 2), index // (count // 2)
    kv_ref[side] = near_ref[...]
    kv_ref[1 - side] = far_ref[...]
    cols = [slice(i * HEAD, (i + 1) * HEAD) for i in range(heads)]
    results = prompt_heads(
        [
            (kv_ref[0, :, at], kv_ref[1, :, at], (pair * heads + i) * PER_HEAD)
            for i, at in enumerate(cols)
        ],
        q_ref, u_ref, qt_ref, ut_ref, rows_ref, stats_ref,
    )
    for i, (at, (key_terms, value_terms, factor, delta)) in enumerate(zip(cols, results)):
        here = slice(i * PER_HEAD * seq, (i + 1) * PER_HEAD * seq)
        scale_ref[0:1, here] = factor
        scale_ref[1:2, here] = delta
        terms_ref[0, :, at] = key_terms.astype(jnp.bfloat16)
        terms_ref[1, :, at] = value_terms.astype(jnp.bfloat16)
    near_terms_ref[...] = terms_ref[side]
    far_terms_ref[...] = terms_ref[1 - side]


def prompt_kernel(count, q_ref, u_ref, qt_ref, ut_ref, rows_ref, stats_ref, *refs):
    blocks = refs[:count]
    scale_ref = refs[count]
    terms_refs = refs[count + 1 : 2 * count + 1]
    kv_ref, terms_ref = refs[2 * count + 1 :]
    me = lax.axis_index("resp")
    seq = q_ref.shape[1]
    features = blocks[0].shape[1]
    for step in range(count):
        kv_ref[sender_to(me, step, count)] = blocks[step][...]

    def prompt_of(first):
        if features >= HEAD:
            at = first % features
            return kv_ref[first // features, :, at : at + HEAD]
        return jnp.concatenate(
            [kv_ref[(first + i) // features] for i in range(0, HEAD, features)], axis=1
        )

    def put(first, value):
        if features >= HEAD:
            at = first % features
            terms_ref[first // features, :, at : at + HEAD] = value
        else:
            for i in range(0, HEAD, features):
                terms_ref[(first + i) // features] = value[:, i : i + features]

    for j in range(KV_HEADS):
        at = slice(j * PER_HEAD * seq, (j + 1) * PER_HEAD * seq)
        head = (prompt_of(j * HEAD), prompt_of((KV_HEADS + j) * HEAD), j * PER_HEAD)
        ((key_terms, value_terms, factor, delta),) = prompt_heads(
            [head], q_ref, u_ref, qt_ref, ut_ref, rows_ref, stats_ref
        )
        scale_ref[0:1, at] = factor
        scale_ref[1:2, at] = delta
        put(j * HEAD, key_terms)
        put((KV_HEADS + j) * HEAD, value_terms)
    for step in range(count):
        terms_refs[step][...] = terms_ref[partner_of(me, step, count)].astype(jnp.bfloat16)


def first_head(step, count, heads):
    if heads == KV_HEADS:
        return 0
    return lax.rem(lax.axis_index("resp") ^ step, count // 2) * heads


def own_grad(step, count, q_ref, u_ref, exp_ref, dots_ref, scale_ref, out_ref):
    seq = q_ref.shape[1]
    heads = scale_ref.shape[1] // (PER_HEAD * seq)
    first = first_head(step, count, heads)
    size = PER_HEAD * HEAD
    for j in range(heads):
        probs, grads = [], []
        for h in range(PER_HEAD):
            here = slice((j * PER_HEAD + h) * seq, (j * PER_HEAD + h + 1) * seq)
            at = pl.ds(pl.multiple_of(((first + j) * PER_HEAD + h) * seq, seq), seq)
            prob = exp_ref[:, at] * scale_ref[0:1, here]
            grad = prob * (dots_ref[:, at] - scale_ref[1:2, here])
            probs.append(prob.astype(jnp.bfloat16))
            grads.append(grad.astype(jnp.bfloat16))
        start = pl.multiple_of((first + j) * size, size)
        cols = slice(j * HEAD, (j + 1) * HEAD)
        keys = dot(jnp.concatenate(grads, axis=1), stacked(q_ref, start), 1, 0) * SCALING
        values = dot(jnp.concatenate(probs, axis=1), stacked(u_ref, start), 1, 0)
        out_ref[0, :, cols] = keys.astype(jnp.bfloat16)
        out_ref[1, :, cols] = values.astype(jnp.bfloat16)


def own_grad_kernel(step, count, *refs):
    own_grad(step, count, *refs)


def last_own_grad_kernel(steps, count, q_ref, u_ref, exp_ref, dots_ref, scale_ref, *refs):
    parts, (gk_ref, gv_ref, held_ref, sems) = refs[: len(steps) - 1], refs[len(steps) - 1 :]
    copies = []

    def store(i, ref):
        heads = ref.shape[2] // HEAD
        first = first_head(steps[i], count, heads) * HEAD
        at = pl.ds(pl.multiple_of(first, HEAD), heads * HEAD)
        for side, target in enumerate((gk_ref, gv_ref)):
            copies.append(pltpu.make_async_copy(ref.at[side], target.at[0, :, at], sems.at[side, i]))
            copies[-1].start()

    for i, ref in enumerate(parts):
        store(i, ref)
    own_grad(steps[-1], count, q_ref, u_ref, exp_ref, dots_ref, scale_ref, held_ref)
    store(len(steps) - 1, held_ref)
    for copy in copies:
        copy.wait()


def sum_kernel(*refs):
    total = refs[0][...].astype(jnp.float32)
    for ref in refs[1:-1]:
        total = total + ref[...].astype(jnp.float32)
    refs[-1][...] = total.astype(jnp.bfloat16)


def weight_kernel(chips, *refs):
    grads, columns, (out_ref, held_ref, sems) = refs[: 2 * chips], refs[2 * chips : 3 * chips], refs[3 * chips :]
    right = jnp.concatenate([ref[side] for side in range(2) for ref in columns], axis=0)
    copies = []
    width = held_ref.shape[0] // sems.shape[0]
    for i in range(sems.shape[0]):
        rows = slice(i * width, (i + 1) * width)
        left = jnp.concatenate([ref[:, rows] for ref in grads], axis=0)
        held_ref[rows] = dot(left, right, 0, 0)
        copies.append(pltpu.make_async_copy(held_ref.at[rows], out_ref.at[rows], sems.at[i]))
        copies[-1].start()
    for copy in copies:
        copy.wait()


def call(kernel, outs, inputs, scratch=(), kinds={}, out_kind=pltpu.VMEM, flops=0, limit=24):
    size = sum(x.size * x.dtype.itemsize for x in list(inputs) + list(outs))
    return pl.pallas_call(
        kernel,
        out_shape=tuple(outs),
        in_specs=[pl.BlockSpec(memory_space=kinds.get(i, pltpu.VMEM)) for i in range(len(inputs))],
        out_specs=tuple(pl.BlockSpec(memory_space=out_kind) for _ in outs),
        scratch_shapes=list(scratch),
        cost_estimate=pl.CostEstimate(flops=flops, bytes_accessed=size, transcendentals=0),
        compiler_params=pltpu.CompilerParams(vmem_limit_bytes=limit << 20),
    )(*inputs)


def shape(dims, dtype):
    return jax.ShapeDtypeStruct(tuple(dims), dtype)


def per_device(
    resps, groups, prompt_hidden, kv_weight, queries, resp_keys, resp_values, upstream, signs, lengths
):
    chips = groups // 2

    def over_resp(value, step):
        pairs = [(i, partner_of(i, step, resps)) for i in range(resps)]
        return lax.ppermute(value, "resp", pairs)

    def over_chips(value, step):
        pairs = [(i, 2 * partner_of(i // 2, step, chips) + 1 - i % 2) for i in range(groups)]
        return lax.ppermute(value, "group", pairs)

    def swap(value):
        return lax.ppermute(value, "group", [(i, i ^ 1) for i in range(groups)])

    seq = queries.shape[1]
    rows, width = prompt_hidden.shape[1:]
    features = kv_weight.shape[0]
    prompt = rows * resps
    unit = 2 * seq * seq * HEAD * HEADS
    bf16, f32 = jnp.bfloat16, jnp.float32
    block = shape((prompt, features), bf16)

    (mask,) = call(mask_kernel, [shape((seq, seq), f32)], [], flops=MASK_FLOPS)
    hidden_blocks = [prompt_hidden] + [over_resp(prompt_hidden, s) for s in range(1, resps)]
    wide = shape((seq, HEADS * seq), f32)
    turned = shape((HEAD, HEADS * seq), bf16)
    queries_t, upstream_t, exps, dots, stats = call(
        own_kernel,
        [turned, turned, wide, wide, shape((8, HEADS * seq), f32)],
        [mask, queries, upstream, resp_keys, resp_values],
        flops=2 * unit,
    )
    (weight_t,) = call(turn_kernel, [shape((width, features), bf16)], [kv_weight])
    prompt_kv, hidden = call(
        functools.partial(project_kernel, resps),
        [block, shape((resps, rows, width), bf16)],
        hidden_blocks + [weight_t],
        flops=2 * prompt * features * width,
    )
    kv_blocks = [prompt_kv] + [over_resp(prompt_kv, s) for s in range(1, resps)]
    (row_weights,) = call(rows_kernel, [shape((1, PER_HEAD * seq), f32)], [signs, lengths])
    shared = [queries, upstream, queries_t, upstream_t, row_weights, stats]
    terms = [None] * resps
    if paired(resps, features):
        half = resps // 2
        steps, scales = tuple(range(half)), []
        for s in steps:
            scale, terms[s], terms[s + half] = call(
                functools.partial(pair_kernel, resps, s),
                [shape((8, features // HEAD * PER_HEAD * seq), f32), block, block],
                [*shared, kv_blocks[s], kv_blocks[s + half]],
                scratch=[pltpu.VMEM((2, prompt, features), bf16)] * 2,
                flops=unit // half,
            )
            scales.append(scale)
    else:
        steps = (0,)
        scale, *terms = call(
            functools.partial(prompt_kernel, resps),
            [shape((8, HEADS * seq), f32)] + [block] * resps,
            [*shared, *kv_blocks],
            scratch=[
                pltpu.VMEM((resps, prompt, features), bf16),
                pltpu.VMEM((resps, prompt, features), f32),
            ],
            flops=unit,
        )
        scales = [scale]
    terms = [terms[0]] + [over_resp(terms[s], s) for s in range(1, resps)]
    columns = width // groups
    spread = call(
        functools.partial(spread_kernel, chips),
        [shape((2, prompt, columns), bf16)] * chips,
        [hidden, swap(hidden)],
    )
    hidden_columns = [spread[0]] + [over_chips(spread[s], s) for s in range(1, chips)]
    (prompt_grad,) = call(sum_kernel, [block], terms)
    grad_columns = [prompt_grad] + [over_chips(prompt_grad, s) for s in range(1, chips)]
    grad_columns = grad_columns + [swap(x) for x in grad_columns]
    halves = []
    for step, scale in zip(steps[:-1], scales):
        (own,) = call(
            functools.partial(own_grad_kernel, step, resps),
            [shape((2, seq, scale.shape[1] // (PER_HEAD * seq) * HEAD), bf16)],
            [queries, upstream, exps, dots, scale],
            flops=2 * unit // len(steps),
        )
        halves.append(own)
    grad_keys, grad_values = call(
        functools.partial(last_own_grad_kernel, steps, resps),
        [shape(resp_keys.shape, bf16), shape(resp_values.shape, bf16)],
        [queries, upstream, exps, dots, scales[-1]] + halves,
        scratch=[
            pltpu.VMEM((2, seq, scales[-1].shape[1] // (PER_HEAD * seq) * HEAD), bf16),
            pltpu.SemaphoreType.DMA((2, len(steps))),
        ],
        out_kind=pl.ANY,
        flops=2 * unit // len(steps),
    )
    (grad_weight,) = call(
        functools.partial(weight_kernel, chips),
        [shape((features, columns), f32)],
        grad_columns + hidden_columns,
        scratch=[
            pltpu.VMEM((features, columns), f32),
            pltpu.SemaphoreType.DMA((max(1, features // HEAD),)),
        ],
        out_kind=pl.ANY,
        flops=2 * groups * prompt * features * columns,
    )
    return (grad_keys, grad_values, grad_weight)


def paired(resps, features):
    return resps > 1 and resps & (resps - 1) == 0 and features % HEAD == 0


MASK_FLOPS = 20_000_000_000


def solution(mesh):
    placed = (
        P("group", "resp", None),
        P("resp", None),
        P("group", "resp", None),
        P("group", "resp", None),
        P("group", "resp", None),
        P("group", "resp", None),
        P("group", "resp"),
        P("group", "resp"),
    )

    def body(*args):
        return per_device(mesh.shape["resp"], mesh.shape["group"], *args)

    return jax.shard_map(
        body,
        mesh=mesh,
        in_specs=placed,
        out_specs=(P("group", "resp", None), P("group", "resp", None), P("resp", "group")),
        check_vma=False,
    )
```
